32 devices in a mesh: mem: 4 (over z), state: 8 (over y, x, core).
Axes of the slice: x: 2, y: 2, z: 4, core: 2. Of those that a mesh axis runs over, the one named last changes fastest.
Arguments:
- anomalies: bfloat16 [64, 32, 32768], P('mem', None, 'state'), may hold values from -0.75 to 0.75
- alpha: bfloat16 [64, 32, 2048], P('mem', None, 'state'), may hold values from -6 to 6
- basis: bfloat16 [2048, 32768], P(None, 'state'), may hold values from -0.1875 to 0.1875
- gradient: bfloat16 [32, 32768], P(None, 'state'), may hold values from -6 to 6
- vertical_root: float32 [32, 32], replicated, may hold values from -1 to 1
- band_gain: float32 [16], replicated, may hold values from 0.25 to 2
- band: int32 [2048], P('state'), may hold values from 0 to 15
- order: int32 [64], replicated, may hold values from 0 to 63, each once
Outputs:
- increment: float32 [32, 32768], P(None, 'state')
- alpha_grad: float32 [64, 32, 2048], P('mem', None, 'state')
The draws below stay inside these ranges and needn't reach their ends.
Inputs may be any that keep to these rules, and one draw needn't show every extreme that they name: `order`: a permutation: every member is named by exactly one slot.
All inputs are finite; a program needn't handle non-finite values.
Results may differ from the reference program's by a relative error of at most 0.0029.
Values may be sent and summed in bfloat16 or wider, within the bound.
No kernel may reach another device: no remote copies, remote signals or barrier semaphores. Data moves between devices by JAX's collectives and lax.ppermute only.
A program may use at most 128 MiB of HBM per device.

```python
import math
import jax
import jax.numpy as jnp
from jax import lax

LEVELS = 32
MODES = 2048
BANDS = 16
MEMBERS = 64
COLUMNS = 32768


def set_ends(result, key, least, top_value):
    spot = [jax.random.randint(jax.random.fold_in(key, axis), (), 0, length) for axis, length in enumerate(result.shape)]
    main_axis = result.shape.index(max(result.shape))
    neighbour = spot[:main_axis] + [(spot[main_axis] + 1) % result.shape[main_axis]] + spot[main_axis + 1:]
    return result.at[tuple(spot)].set(least).at[tuple(neighbour)].set(top_value)


def raised(values, key, source, target, blocks, factor):
    owner, partner = [(jnp.arange(values.shape[dim]) // (values.shape[dim] // blocks)).reshape([-1 if axis == dim else 1 for axis in range(values.ndim)]) for dim in (source, target)]
    chosen = jax.random.permutation(key, blocks)[partner]
    strong = (owner == chosen) | (owner == (partner + blocks // 2) % blocks)
    return jnp.where(strong, factor * values, values)


def steps_of(own_key, extent, shards, low, top_value):
    gain, own = 1.0, jax.random.fold_in(own_key, 6)
    for axis_at, parts in shards:
        heights = jnp.exp(jax.random.uniform(jax.random.fold_in(own, axis_at), (parts,), jnp.float32, low / len(shards), top_value / len(shards)))
        gain = gain * jnp.repeat(heights, extent[axis_at] // parts).reshape([-1 if axis == axis_at else 1 for axis in range(len(extent))])
    return gain


def normal_values(own_key, shape, spread, reach, cuts=(), kind=jnp.bfloat16):
    result = jax.random.normal(own_key, shape, jnp.float32) * spread
    if len(cuts) > 0:
        result = steps_of(own_key, shape, cuts, -0.22, 0.18) * result
    return jnp.clip(result, min=-reach, max=reach).astype(kind)


def noise_with(rng, dims, scale, most, pieces, heavy, kind=jnp.bfloat16):
    array = scale * jax.random.normal(rng, dims, jnp.float32)
    if pieces:
        array = array * steps_of(rng, dims, pieces, -0.22, 0.18)
    return jnp.clip(raised(array, jax.random.fold_in(rng, 3), *heavy), -most, most).astype(kind)


def setup_inputs(seed: int = 0) -> dict:
    arg_keys = jax.random.split(jax.random.key(seed), 9)
    return {
        "anomalies": normal_values(arg_keys[0], (MEMBERS, LEVELS, COLUMNS), 0.125, 0.75, ((0, 4), (2, 8))),
        "alpha": normal_values(arg_keys[1], (MEMBERS, LEVELS, MODES), 1.0, 6.0, ((0, 4), (2, 8))),
        "basis": noise_with(arg_keys[2], (MODES, COLUMNS), MODES ** -0.5, 0.1875, ((1, 8),), (1, 0, 8, 2.0)),
        "gradient": normal_values(arg_keys[3], (LEVELS, COLUMNS), 1.0, 6.0, ((1, 8),)),
        "vertical_root": normal_values(arg_keys[4], (LEVELS, LEVELS), LEVELS ** -0.5, 1.0, (), jnp.float32),
        "band_gain": jnp.clip(jnp.exp(jax.random.uniform(arg_keys[5], (BANDS,), jnp.float32, math.log(0.25), math.log(2.0))), 0.25, 2.0),
        "band": set_ends(jax.random.randint(arg_keys[6], (MODES,), 0, BANDS), jax.random.fold_in(arg_keys[6], 1), 0, BANDS - 1).astype(jnp.int32),
        "order": jax.random.permutation(arg_keys[7], MEMBERS).astype(jnp.int32),
    }


def reference(anomalies, alpha, basis, gradient, vertical_root, band_gain, band, order):
    high = lax.Precision.HIGHEST
    onehot = (band[:, None] == jnp.arange(BANDS, dtype=jnp.int32)[None, :]).astype(jnp.float32)
    filter_gain = jnp.sum(onehot * band_gain[None, :], axis=1)
    coef = jnp.einsum("ab,jbk->jak", vertical_root, alpha.astype(jnp.float32), precision=high)
    coef = (coef * filter_gain[None, None, :]).astype(jnp.bfloat16)
    inverse = jnp.zeros((MEMBERS,), jnp.int32).at[order].set(jnp.arange(MEMBERS, dtype=jnp.int32))
    member_coef = coef[inverse]
    grad_float = gradient.astype(jnp.float32)

    def one_member(running, member_items):
        member_anom, member_c = member_items
        member_field = jnp.dot(member_c, basis, preferred_element_type=jnp.float32)
        running = running + member_anom.astype(jnp.float32) * member_field
        weighted = (member_anom.astype(jnp.float32) * grad_float).astype(jnp.bfloat16)
        projected = lax.dot_general(weighted, basis, (((1,), (1,)), ((), ())), preferred_element_type=jnp.float32)
        return running, projected

    increment, projected = lax.scan(one_member, jnp.zeros((LEVELS, COLUMNS), jnp.float32), (anomalies, member_coef))
    slot_proj = projected[order]
    alpha_grad = jnp.einsum("ab,jak->jbk", vertical_root, slot_proj, precision=high) * filter_gain[None, None, :]
    return increment, alpha_grad
```

```python
import jax
import jax.numpy as jnp
from jax import lax
from jax.experimental import pallas as pl
from jax.experimental.pallas import tpu as pltpu
from jax.sharding import PartitionSpec as P


def project_kernel(rows_ref, anomalies_ref, gradient_ref, basis_ref, given_ref, kept_ref, weighted_ref):
    step = pl.program_id(0)
    levels = gradient_ref.shape[0]

    @pl.when(step == 0)
    def _():
        scale = gradient_ref[...].astype(jnp.float32)
        for member in range(anomalies_ref.shape[0]):
            value = anomalies_ref[member].astype(jnp.float32) * scale
            weighted_ref[member * levels : (member + 1) * levels, :] = value.astype(jnp.bfloat16)

    def sums():
        return lax.dot_general(
            weighted_ref[...], basis_ref[...], (((1,), (1,)), ((), ())), preferred_element_type=jnp.float32
        )

    half = pl.num_programs(0) // 2

    @pl.when(step < half)
    def _():
        given_ref[0] = sums()

    @pl.when(step >= half)
    def _():
        kept_ref[0] = sums()


def project(anomalies, gradient, basis, rows, width):
    members, levels, columns = anomalies.shape
    height, count = members * levels, rows.shape[0]
    half = count // 2
    result = jax.ShapeDtypeStruct((half, height, width), jnp.float32)
    return pl.pallas_call(
        project_kernel,
        grid_spec=pltpu.PrefetchScalarGridSpec(
            num_scalar_prefetch=1,
            grid=(count,),
            in_specs=[
                pl.BlockSpec((members, levels, columns), lambda g, rows: (0, 0, 0)),
                pl.BlockSpec((levels, columns), lambda g, rows: (0, 0)),
                pl.BlockSpec((width, columns), lambda g, rows: (rows[g], 0)),
            ],
            out_specs=[
                pl.BlockSpec((1, height, width), lambda g, rows: (jnp.minimum(g, half - 1), 0, 0)),
                pl.BlockSpec((1, height, width), lambda g, rows: (jnp.maximum(g - half, 0), 0, 0)),
            ],
            scratch_shapes=[pltpu.VMEM((height, columns), jnp.bfloat16)],
        ),
        out_shape=[result, result],
        cost_estimate=pl.CostEstimate(
            flops=2 * height * columns * width * count,
            bytes_accessed=2 * (height * columns + width * columns * count),
            transcendentals=0,
        ),
        name="project",
    )(rows, anomalies, gradient, basis)


def synthesize_kernel(levels, rows_ref, places_ref, *refs):
    blocks, (basis_ref, anomalies_ref, out_ref) = refs[:-3], refs[-3:]
    total = None
    for index, block in enumerate(blocks):
        width = block.shape[1]
        rows = basis_ref[pl.ds(rows_ref[index] * width, width), :]
        term = jnp.dot(block[...], rows, preferred_element_type=jnp.float32)
        total = term if total is None else total + term
    result = None
    for member in range(anomalies_ref.shape[0]):
        term = anomalies_ref[member].astype(jnp.float32) * total[member * levels : (member + 1) * levels]
        result = term if result is None else result + term
    out_ref[0] = result


def synthesize(blocks, basis, anomalies, rows, places, parts, tile):
    members, levels, columns = anomalies.shape
    piece = columns // parts
    steps = piece // tile
    count = places.shape[0]
    block_spec = pl.BlockSpec(blocks[0].shape, lambda p, t, rows, places: (0, 0))
    return pl.pallas_call(
        lambda *refs: synthesize_kernel(levels, *refs),
        grid_spec=pltpu.PrefetchScalarGridSpec(
            num_scalar_prefetch=2,
            grid=(count, steps),
            in_specs=[block_spec] * len(blocks)
            + [
                pl.BlockSpec((basis.shape[0], tile), lambda p, t, rows, places: (0, places[p] * steps + t)),
                pl.BlockSpec((members, levels, tile), lambda p, t, rows, places: (0, 0, places[p] * steps + t)),
            ],
            out_specs=pl.BlockSpec((1, levels, tile), lambda p, t, rows, places: (p, 0, t)),
        ),
        out_shape=jax.ShapeDtypeStruct((count, levels, piece), jnp.float32),
        cost_estimate=pl.CostEstimate(
            flops=2 * members * levels * basis.shape[0] * piece * count,
            bytes_accessed=2 * (basis.shape[0] + members * levels) * piece * count,
            transcendentals=0,
        ),
        name="synthesize",
    )(rows, places, *blocks, basis, anomalies)


def two_parts(value):
    high = lax.reduce_precision(value, 8, 7)
    return high.astype(jnp.bfloat16), (value - high).astype(jnp.bfloat16)


def mixing(values, row_ids, column_ids):
    levels = values.shape[0]
    same = row_ids[:, None] == column_ids[None, :]
    tiled = jnp.tile(values, (1, column_ids.shape[0] // levels))
    wide = jnp.tile(tiled, (row_ids.shape[0] // levels, 1))
    return [jnp.where(same, part, jnp.zeros((), jnp.bfloat16)) for part in two_parts(wide)]


def on_device(anomalies, alpha, basis, gradient, vertical_root, band_gain, band, order):
    bf16, f32 = jnp.bfloat16, jnp.float32
    mem_count, state_count = lax.axis_size("mem"), lax.axis_size("state")
    mem_rank, state_rank = lax.axis_index("mem"), lax.axis_index("state")
    member_dev, levels, columns = anomalies.shape
    width = alpha.shape[2]
    height = member_dev * levels
    pairs = state_count // 2
    spot, core = state_rank // 2, state_rank % 2

    def along_mem(value, step):
        return lax.ppermute(value, "mem", [(i, (i + step) % mem_count) for i in range(mem_count)])

    def across_pairs(value, step):
        return lax.ppermute(
            value, "state", [(i, (i + 2 * step) % state_count) for i in range(state_count)]
        )

    def other_core(value):
        return lax.ppermute(value, "state", [(i, i ^ 1) for i in range(state_count)])

    def gather_mem(value):
        return jnp.concatenate([value] + [along_mem(value, step) for step in range(1, mem_count)], axis=0)

    slots = gather_mem(alpha.reshape(height, width))

    onehot = (band[:, None] == jnp.arange(band_gain.shape[0], dtype=jnp.int32)[None, :]).astype(f32)
    filter_gain = jnp.sum(onehot * band_gain[None, :], axis=1)
    sources = (mem_rank - jnp.arange(mem_count, dtype=jnp.int32)) % mem_count
    slot_members = order.reshape(mem_count, member_dev)
    held = (sources[:, None] * member_dev + jnp.arange(member_dev, dtype=jnp.int32)[None, :]).reshape(-1)
    own = mem_rank * member_dev + jnp.arange(member_dev, dtype=jnp.int32)
    spread = lambda ids: jnp.repeat(ids, levels)
    to_members = mixing(vertical_root, spread(own), spread(slot_members[sources].reshape(-1)))
    to_slots = mixing(vertical_root.T, spread(slot_members[mem_rank]), spread(held))

    targets = (spot + jnp.arange(pairs, dtype=jnp.int32)) % pairs
    given, kept = project(
        anomalies, gradient, basis, jnp.concatenate([2 * targets + 1 - core, 2 * targets + core]), width
    )
    taken = other_core(given)
    chip_sums = [kept[step] + taken[step] for step in range(pairs)]
    projected = chip_sums[0]
    arrived = [across_pairs(chip_sums[step].astype(bf16), step) for step in range(1, pairs)]
    for block in arrived:
        projected = projected + block.astype(f32)

    coef = sum(jnp.dot(part, slots, preferred_element_type=f32) for part in to_members)
    coef = (coef * filter_gain[None, :]).astype(bf16)
    own_core = [coef] + [across_pairs(coef, step) for step in range(1, pairs)]
    blocks = own_core + [other_core(block) for block in own_core]
    origins = (spot - jnp.arange(pairs, dtype=jnp.int32)) % pairs
    rows = jnp.concatenate([2 * origins + core, 2 * origins + 1 - core])
    tile = min(512, columns // mem_count)
    places = (mem_rank + jnp.arange(mem_count, dtype=jnp.int32)) % mem_count
    far = synthesize(blocks, basis, anomalies, rows, places[1:], mem_count, tile)
    piece_sum = synthesize(blocks, basis, anomalies, rows, places[:1], mem_count, tile)[0]
    shares = [along_mem(far[step - 1].astype(bf16), step) for step in range(1, mem_count)]
    for share in shares:
        piece_sum = piece_sum + share.astype(f32)
    summed = piece_sum.astype(bf16)
    all_pieces = jnp.stack([summed] + [along_mem(summed, step) for step in range(1, mem_count)])
    increment = jnp.concatenate(
        [all_pieces[(mem_rank - place) % mem_count] for place in range(mem_count)], axis=1
    ).astype(f32)

    member_projections = gather_mem(projected.astype(bf16))
    alpha_grad = sum(jnp.dot(part, member_projections, preferred_element_type=f32) for part in to_slots)
    alpha_grad = (alpha_grad * filter_gain[None, :]).reshape(member_dev, levels, width)
    return (increment, alpha_grad)


def solution(mesh):
    return jax.shard_map(
        on_device,
        mesh=mesh,
        in_specs=(
            P("mem", None, "state"),
            P("mem", None, "state"),
            P(None, "state"),
            P(None, "state"),
            P(),
            P(),
            P("state"),
            P(),
        ),
        out_specs=(P(None, "state"), P("mem", None, "state")),
        check_vma=False,
    )
```
